32 devices in a mesh: gx: 8 (over y, x, core), gy: 4 (over z).
Axes of the slice: x: 2, y: 2, z: 4, core: 2. Of those that a mesh axis runs over, the one named last changes fastest.
Arguments:
- flow_field: bfloat16 [4, 64, 1024, 512], P(None, None, ('gx', 'gy')), may hold values from -6 to 6
- cotangent: bfloat16 [4, 64, 1024, 512], P(None, None, ('gx', 'gy')), may hold values from -2 to 2
- spectral_weight: bfloat16 [128, 64, 64, 128], P(('gx', 'gy')), may hold values from -0.75 to 0.75
- local_weight: bfloat16 [64, 64], replicated, may hold values from -0.75 to 0.75
- channel_bias: float32 [64], replicated, may hold values from -3 to 3
Outputs:
- output_field: bfloat16 [4, 64, 1024, 512], P(None, None, ('gx', 'gy'))
- grad_field: bfloat16 [4, 64, 1024, 512], P(None, None, ('gx', 'gy'))
- grad_spectral: float32 [128, 64, 64, 128], P(('gx', 'gy'))
The draws below stay inside these ranges and needn't reach their ends.
All inputs are finite; a program needn't handle non-finite values.
Results may differ from the reference program's by a relative error of at most 0.014.
Values may be sent and summed in bfloat16 or wider, within the bound.
A program may use at most 128 MiB of HBM per device.

```python
import math
import jax
import jax.numpy as jnp
from jax import lax

C = 64
NX = 1024
NY = 512
MODES = 64
Z = 4
KC = 128


def level_of(stream_key, dims, cuts, low, high):
    level, own = 1.0, jax.random.fold_in(stream_key, 6)
    for axis_at, blocks in cuts:
        draws = jnp.exp(jax.random.uniform(jax.random.fold_in(own, axis_at), (blocks,), jnp.float32, low / len(cuts), high / len(cuts)))
        level = level * jnp.repeat(draws, dims[axis_at] // blocks).reshape([-1 if axis == axis_at else 1 for axis in range(len(dims))])
    return level


def centred(key, shape, width, bound, cuts=(), kind=jnp.bfloat16):
    factor_of = level_of(key, shape, cuts, -0.22, 0.18) if cuts else 1.0
    values = jax.random.normal(key, shape, jnp.float32) * width * factor_of
    return jnp.minimum(jnp.maximum(values, -bound), bound).astype(kind)


def setup_inputs(seed: int = 0) -> dict:
    splits = jax.random.split(jax.random.key(seed), 6)
    flow_field = centred(splits[0], (Z, C, NX, NY), 1.0, 6.0, ((2, 32),))
    cotangent = centred(splits[1], (Z, C, NX, NY), 0.3, 2.0, ((2, 32),))
    spectral_weight = centred(splits[2], (KC, C, C, KC), C ** -0.5, 0.75, ((0, 32),))
    local_weight = centred(splits[3], (C, C), C ** -0.5, 0.75)
    channel_bias = centred(splits[4], (C,), 0.5, 3.0, (), jnp.float32)
    return dict(flow_field=flow_field, cotangent=cotangent, spectral_weight=spectral_weight, local_weight=local_weight, channel_bias=channel_bias)


root_half = 0.7071067811865476
density_norm = 0.3989422804014327

def basis_table(positions, columns, cells, kept, factor):
    frequency = jnp.where(columns < kept, columns, columns - kept + 1)
    phases = positions[:, None] * frequency[None, :] % cells
    angles = phases.astype(jnp.float32) * (2.0 * math.pi / cells)
    values = jnp.where(columns[None, :] < kept, jnp.cos(angles), jnp.sin(angles))
    return (values * factor).astype(jnp.bfloat16)

def gelu_slope(values):
    cumulative = 0.5 * (1.0 + lax.erf(values * root_half))
    density = jnp.exp(-0.5 * values * values) * density_norm
    return cumulative + values * density

def reference(flow_field, cotangent, spectral_weight, local_weight, channel_bias):
    columns = jnp.arange(2 * MODES, dtype=jnp.int32)
    rows_x = jnp.arange(NX, dtype=jnp.int32)
    rows_y = jnp.arange(NY, dtype=jnp.int32)
    fwd_x = basis_table(rows_x, columns, NX, MODES, math.sqrt(2.0 / NX)).astype(jnp.float32)
    fwd_y = basis_table(rows_y, columns, NY, MODES, math.sqrt(2.0 / NY)).astype(jnp.float32)
    inv_x = basis_table(rows_x, columns, NX, MODES, math.sqrt(1.0 / MODES)).astype(jnp.float32)
    inv_y = basis_table(rows_y, columns, NY, MODES, math.sqrt(1.0 / MODES)).astype(jnp.float32)
    weights = spectral_weight.astype(jnp.float32)
    mixing = local_weight.astype(jnp.float32)

    def to_modes(plane, table_x, table_y):
        along = jnp.einsum('cxy,yj->cjx', plane.astype(jnp.float32), table_y).astype(jnp.bfloat16)
        return jnp.einsum('cjx,xk->cjk', along.astype(jnp.float32), table_x).astype(jnp.bfloat16)

    def to_space(modal, table_x, table_y):
        partial_x = jnp.einsum('cjk,xk->cjx', modal.astype(jnp.float32), table_x).astype(jnp.bfloat16)
        return jnp.einsum('cjx,yj->cxy', partial_x.astype(jnp.float32), table_y, precision=lax.Precision.HIGHEST)

    def plane_step(accum, inputs):
        plane, grad_out = inputs
        coeffs = to_modes(plane, fwd_x, fwd_y)
        mixed = jnp.einsum('ijk,jiok->ojk', coeffs.astype(jnp.float32), weights).astype(jnp.bfloat16)
        spectral = to_space(mixed, inv_x, inv_y)
        pointwise = jnp.einsum('ixy,io->oxy', plane.astype(jnp.float32), mixing)
        pre_activation = spectral + pointwise + channel_bias[:, None, None]
        output_plane = jax.nn.gelu(pre_activation, approximate=False).astype(jnp.bfloat16)
        grad_pre = (grad_out.astype(jnp.float32) * gelu_slope(pre_activation)).astype(jnp.bfloat16)
        grad_mixed = to_modes(grad_pre, inv_x, inv_y)
        accum = accum + jnp.einsum('ijk,ojk->jiok', coeffs.astype(jnp.float32), grad_mixed.astype(jnp.float32))
        grad_coeffs = jnp.einsum('ojk,jiok->ijk', grad_mixed.astype(jnp.float32), weights).astype(jnp.bfloat16)
        backward = to_space(grad_coeffs, fwd_x, fwd_y)
        grad_plane = (backward + jnp.einsum('oxy,io->ixy', grad_pre.astype(jnp.float32), mixing)).astype(jnp.bfloat16)
        return (accum, (output_plane, grad_plane))
    start = jnp.zeros((2 * MODES, C, C, 2 * MODES), jnp.float32)
    grad_spectral, (output_field, grad_field) = lax.scan(plane_step, start, (flow_field, cotangent))
    return (output_field, grad_field, grad_spectral)
```

```python
import math

import jax
import jax.numpy as jnp
import numpy as np
from jax import lax
from jax.sharding import PartitionSpec as P

root_half = 0.7071067811865476
density_norm = 0.3989422804014327


def basis_table(cells, cols, factor):
    kept = cols // 2
    columns = np.arange(cols)
    frequency = np.where(columns < kept, columns, columns - kept + 1)
    phases = np.arange(cells)[:, None] * frequency[None, :] % cells
    angles = phases.astype(np.float32) * np.float32(2.0 * math.pi / cells)
    values = np.where(columns[None, :] < kept, np.cos(angles), np.sin(angles))
    return jnp.asarray((values * np.float32(factor)).astype(jnp.bfloat16))


def gelu_slope(values):
    cumulative = 0.5 * (1.0 + lax.erf(values * root_half))
    density = jnp.exp(-0.5 * values * values) * density_norm
    return cumulative + values * density


def to_owners(modal_rows):
    return lax.all_to_all(modal_rows, ("gx", "gy"), split_axis=0, concat_axis=1, tiled=True)


def to_slabs(modal_part):
    return lax.all_to_all(modal_part, ("gx", "gy"), split_axis=1, concat_axis=0, tiled=True)


def contract(spec, left, right):
    return jnp.einsum(spec, left, right, preferred_element_type=jnp.float32)


def shards(flow_field, cotangent, spectral_weight, local_weight, channel_bias):
    devices = lax.axis_size("gx") * lax.axis_size("gy")
    planes, channels, slab_rows, cells_along = flow_field.shape
    cells_across = slab_rows * devices
    own_cols = spectral_weight.shape[0]
    mode_cols = spectral_weight.shape[3]
    kept_modes = mode_cols // 2
    both = planes * channels
    scale_inv = math.sqrt(1.0 / kept_modes)
    fwd_x = basis_table(cells_across, mode_cols, math.sqrt(2.0 / cells_across))
    fwd_y = basis_table(cells_along, mode_cols, math.sqrt(2.0 / cells_along))
    inv_x = basis_table(cells_across, mode_cols, scale_inv)
    inv_y = basis_table(cells_along, mode_cols, scale_inv)

    def to_modes(field, table_x, table_y):
        rows = contract("axy,yj->jxa", field.reshape(both, slab_rows, cells_along), table_y)
        received = to_owners(rows.astype(jnp.bfloat16))
        modes = contract("jxa,xk->jka", received, table_x).astype(jnp.bfloat16)
        return modes.reshape(own_cols, mode_cols, planes, channels)

    def to_rows(modes, table_x):
        merged = modes.reshape(own_cols, mode_cols, both)
        return to_slabs(contract("jka,xk->jxa", merged, table_x).astype(jnp.bfloat16))

    def to_space(rows, table_y):
        field = contract("jxa,yj->axy", rows, table_y)
        return field.reshape(planes, channels, slab_rows, cells_along)

    coeffs = to_modes(flow_field, fwd_x, fwd_y)
    mixed = contract("jkzi,jiok->jkzo", coeffs, spectral_weight).astype(jnp.bfloat16)
    gathered = to_rows(mixed, inv_x)
    spectral = to_space(gathered, inv_y)
    pointwise = contract("zixy,io->zoxy", flow_field, local_weight)
    pre_activation = spectral + pointwise + channel_bias[None, :, None, None]
    output_field = jax.nn.gelu(pre_activation, approximate=False).astype(jnp.bfloat16)
    grad_pre = (cotangent.astype(jnp.float32) * gelu_slope(pre_activation)).astype(jnp.bfloat16)
    grad_mixed = to_modes(grad_pre, inv_x, inv_y)
    grad_coeffs = contract("jkzo,jiok->jkzi", grad_mixed, spectral_weight).astype(jnp.bfloat16)
    gathered_back = to_rows(grad_coeffs, fwd_x)
    grad_spectral = contract("jkzi,jkzo->jiok", coeffs, grad_mixed)
    backward = to_space(gathered_back, fwd_y)
    through_local = contract("zoxy,io->zixy", grad_pre, local_weight)
    grad_field = (backward + through_local).astype(jnp.bfloat16)
    return (output_field, grad_field, grad_spectral)


def solution(mesh):
    placed = (
        P(None, None, ("gx", "gy"), None),
        P(None, None, ("gx", "gy"), None),
        P(("gx", "gy"), None, None, None),
        P(),
        P(),
    )
    return jax.shard_map(
        shards,
        mesh=mesh,
        in_specs=placed,
        out_specs=(
            P(None, None, ("gx", "gy"), None),
            P(None, None, ("gx", "gy"), None),
            P(("gx", "gy"), None, None, None),
        ),
        check_vma=False,
    )
```
